512 devices in a mesh: bank: 32 (over y, x), zero: 16 (over z, core).
Axes of the slice: x: 4, y: 8, z: 8, core: 2. Of those that a mesh axis runs over, the one named last changes fastest.
Arguments:
- master_down: float32 [64, 1024, 2048], P('bank', None, 'zero'), may hold values from -0.25 to 0.25
- router_weight: float32 [2048, 64], P('zero', 'bank'), may hold values from -0.125 to 0.125
- router_gain: float32 [2048], P('zero'), may hold values from 0.25 to 1.75
Outputs:
- final_down: bfloat16 [64, 1024, 2048], P('bank')
- scale_down: float32 [64, 1024], P('bank')
- serve_router: bfloat16 [2048, 64], replicated
The draws below stay inside these ranges and needn't reach their ends.
All inputs are finite; a program needn't handle non-finite values. Where the reference program divides by a largest or mean magnitude, that divisor is 1e-20 or more.
Results may differ from the reference program's by a relative error of at most 0.001.
Values may be sent and summed in bfloat16 or wider, within the bound.
A program may use at most 64 MiB of HBM per device.

```python
import jax
import jax.numpy as jnp

EXPERTS = 64
D_MODEL = 2048
D_EXPERT = 1024


def spiked(array, stream_key, source, target, shards_of, factor):
    def block_of(dim):
        return (jnp.arange(array.shape[dim]) // (array.shape[dim] // shards_of)).reshape((-1,) + (1,) * (array.ndim - 1 - dim))

    first = jax.random.permutation(stream_key, shards_of)[block_of(target)]
    second = (block_of(target) + shards_of // 2) % shards_of
    return jnp.where((block_of(source) == first) | (block_of(source) == second), factor * array, array)


def block_levels(rng, shape, pieces, least, high):
    loudness = 1.0
    for dim, blocks in pieces:
        steps = jax.random.uniform(jax.random.fold_in(jax.random.fold_in(rng, 6), dim), (blocks,), jnp.float32, least / len(pieces), high / len(pieces))
        loudness = loudness * jnp.repeat(jnp.exp(steps), shape[dim] // blocks).reshape((-1,) + (1,) * (len(shape) - 1 - dim))
    return loudness


def bell_draw(rng, extent, deviation, bound, pieces=(), dtype=jnp.bfloat16):
    drawn = deviation * jax.random.normal(rng, extent, jnp.float32)
    if pieces:
        drawn = drawn * block_levels(rng, extent, pieces, -0.22, 0.18)
    return jnp.clip(drawn, -bound, bound).astype(dtype)


def gaussian_with(rng, shape, scale, limit, pieces, heavy, dtype=jnp.bfloat16):
    entries = scale * jax.random.normal(rng, shape, jnp.float32)
    if pieces:
        entries = entries * block_levels(rng, shape, pieces, -0.22, 0.18)
    return jnp.clip(spiked(entries, jax.random.fold_in(rng, 3), *heavy), -limit, limit).astype(dtype)


def setup_inputs(seed: int = 0) -> dict:
    splits = jax.random.split(jax.random.key(seed), 4)
    master_down = gaussian_with(splits[0], (EXPERTS, D_EXPERT, D_MODEL), D_EXPERT ** -0.5, 0.25, ((0, 32), (2, 16)), (2, 1, 16, 2.0), jnp.float32)
    router_weight = bell_draw(splits[1], (D_MODEL, EXPERTS), D_MODEL ** -0.5, 0.125, ((0, 16), (1, 32)), jnp.float32)
    router_gain = jnp.clip(1.0 + 0.15 * jax.random.normal(splits[2], (D_MODEL,), jnp.float32), 0.25, 1.75)
    return dict(master_down=master_down, router_weight=router_weight, router_gain=router_gain)


def reference(master_down, router_weight, router_gain):
    scale_down = jnp.max(jnp.abs(master_down), axis=2)
    final_down = (master_down / jnp.expand_dims(scale_down, 2)).astype(jnp.bfloat16)
    serve_router = (router_weight * router_gain[:, None]).astype(jnp.bfloat16)
    return final_down, scale_down, serve_router
```

```python
import functools

import jax
import jax.numpy as jnp
from jax import lax
from jax.experimental import pallas as pl
from jax.experimental.pallas import tpu as pltpu
from jax.sharding import PartitionSpec as P

MESH = pl.DeviceIdType.MESH
LANES = 128
CHUNK = 256
LOADS = 4
PUTS = 8


def kernel(
    banks, zeros, w_hbm, r_hbm, g_hbm, out, scale, router,
    w, r, g, maxima, rows, parts, columns,
    load_sem, max_send, max_recv, part_send, part_recv, col_send, col_recv,
    ring_send, ring_recv, pair_send, pair_recv,
):
    total = w_hbm.shape[0]
    chunks, blocks = total // CHUNK, total // LANES
    chips = zeros // 2
    half = chunks // 2
    bank, zero = lax.axis_index("bank"), lax.axis_index("zero")
    chip, core = zero // 2, lax.rem(zero, 2)
    partner = chip * 2 + 1 - core

    def shard_of(distance):
        return lax.rem(chip + distance + chips, chips) * 2 + core

    right, left = shard_of(1), shard_of(-1)

    barrier = pltpu.get_barrier_semaphore()
    share = total // LOADS

    def load(i):
        at = pl.ds(i * share, share)
        return pltpu.make_async_copy(w_hbm.at[at], w.at[at], load_sem.at[i])

    load_r = pltpu.make_async_copy(r_hbm, r, load_sem.at[LOADS])
    load_g = pltpu.make_async_copy(g_hbm, g, load_sem.at[LOADS + 1])
    for i in range(LOADS):
        load(i).start()
    load_r.start()
    load_g.start()

    @pl.loop(1, zeros)
    def _(d):
        pl.semaphore_signal(
            barrier, inc=1, device_id={"zero": lax.rem(zero + d, zeros)}, device_id_type=MESH
        )

    @pl.loop(1, banks)
    def _(d):
        pl.semaphore_signal(
            barrier, inc=1, device_id={"bank": lax.rem(bank + d, banks)}, device_id_type=MESH
        )

    for i in range(LOADS):
        load(i).wait()
        for j in range(i * blocks // LOADS, (i + 1) * blocks // LOADS):
            block = jnp.abs(w[j * LANES : (j + 1) * LANES, :])
            maxima[zero, j : j + 1, :] = jnp.max(block.T, axis=0, keepdims=True)
    load_r.wait()
    load_g.wait()
    product = r[...] * g[...]
    parts[zero, :, 0:LANES] = product[0:1]
    parts[zero, :, LANES : 2 * LANES] = product[1:2]

    pl.semaphore_wait(barrier, zeros - 1 + banks - 1)

    def send_max(peer):
        return pltpu.make_async_remote_copy(
            src_ref=maxima.at[zero], dst_ref=maxima.at[zero],
            send_sem=max_send.at[peer], recv_sem=max_recv.at[zero],
            device_id={"zero": peer}, device_id_type=MESH,
        )

    def take_max(peer):
        return pltpu.make_async_remote_copy(
            src_ref=maxima.at[peer], dst_ref=maxima.at[peer],
            send_sem=max_send.at[peer], recv_sem=max_recv.at[peer],
            device_id={"zero": peer}, device_id_type=MESH,
        )

    def send_part(peer):
        return pltpu.make_async_remote_copy(
            src_ref=parts.at[zero], dst_ref=parts.at[zero],
            send_sem=part_send.at[peer], recv_sem=part_recv.at[zero],
            device_id={"zero": peer}, device_id_type=MESH,
        )

    def take_part(peer):
        return pltpu.make_async_remote_copy(
            src_ref=parts.at[peer], dst_ref=parts.at[peer],
            send_sem=part_send.at[peer], recv_sem=part_recv.at[peer],
            device_id={"zero": peer}, device_id_type=MESH,
        )

    offsets = sorted(range(1, chips), key=lambda o: -min(o, chips - o))
    peers = [lax.rem(chip + o, chips) * 2 + c for o in offsets for c in (core, 1 - core)]
    peers.append(partner)
    for peer in peers:
        send_max(peer).start()
    for peer in peers:
        send_part(peer).start()
    for peer in reversed(peers):
        take_max(peer).wait_recv()

    most = maxima[0]
    for i in range(1, zeros):
        most = jnp.maximum(most, maxima[i])
    rows[...] = most
    half_blocks = blocks // 2
    for j in range(blocks):
        e, at = j // half_blocks, (j % half_blocks) * LANES
        scale[e : e + 1, at : at + LANES] = most[j : j + 1, :]

    def piece(shard, k):
        return out.at[
            pl.ds(pl.multiple_of(k * CHUNK, CHUNK), CHUNK),
            pl.ds(pl.multiple_of(shard * LANES, LANES), LANES),
        ]

    def hop(way, step, shard, k):
        return pltpu.make_async_remote_copy(
            src_ref=piece(shard, k), dst_ref=piece(shard, k),
            send_sem=ring_send.at[way, step, k], recv_sem=ring_recv.at[way, step, k],
            device_id={"zero": (right, left)[way]}, device_id_type=MESH,
        )

    def pair(slot, shard, k):
        return pltpu.make_async_remote_copy(
            src_ref=piece(shard, k), dst_ref=piece(shard, k),
            send_sem=pair_send.at[slot, k], recv_sem=pair_recv.at[slot, k],
            device_id={"zero": partner}, device_id_type=MESH,
        )

    @pl.loop(0, chunks)
    def _(k):
        for i in range(CHUNK // LANES):
            j = k * (CHUNK // LANES) + i
            at = pl.ds(pl.multiple_of(j * LANES, LANES), LANES)
            by = jnp.broadcast_to(rows[pl.ds(j, 1), :], (LANES, LANES)).T
            to = pl.ds(pl.multiple_of(zero * LANES, LANES), LANES)
            out[at, to] = (w[at, :] / by).astype(jnp.bfloat16)
        hop(0, 0, zero, k).start()
        hop(1, 0, zero, k).start()
        pair(0, zero, k).start()

    for peer in peers:
        take_part(peer).wait_recv()
    tile = pl.multiple_of(bank * 2 * zeros, 2 * zeros)
    for i in range(zeros):
        columns[pl.ds(tile + i, 1), :] = parts[i, :, 0:LANES]
        columns[pl.ds(tile + zeros + i, 1), :] = parts[i, :, LANES : 2 * LANES]

    def column_copy(owner, peer):
        at = pl.ds(pl.multiple_of(owner * 2 * zeros, 2 * zeros), 2 * zeros)
        return pltpu.make_async_remote_copy(
            src_ref=columns.at[at], dst_ref=columns.at[at],
            send_sem=col_send.at[peer], recv_sem=col_recv.at[owner],
            device_id={"bank": peer}, device_id_type=MESH,
        )

    @pl.loop(1, banks)
    def _(d):
        column_copy(bank, lax.rem(bank + d, banks)).start()

    def forward(way, step, k, onward):
        distance = -step if way == 0 else step
        shard = shard_of(distance)
        slot = distance % chips
        hop(way, step - 1, shard, k).wait_recv()
        if onward:
            hop(way, step, shard, k).start()
        pair(slot, shard, k).start()

    def finish_router():
        @pl.loop(1, banks)
        def _(d):
            owner = lax.rem(bank + d, banks)
            column_copy(owner, owner).wait_recv()

        for i in range(zeros):
            router[:, i * LANES : (i + 1) * LANES] = columns[
                pl.ds(i, 2 * banks, stride=zeros), :
            ].astype(jnp.bfloat16)

    far = chips // 2
    for step in range(1, far):
        if step < far - 1:

            @pl.loop(0, chunks)
            def _(k):
                forward(0, step, k, True)
                forward(1, step, k, True)
        else:

            @pl.loop(0, half)
            def _(k):
                forward(0, step, k, True)
                forward(1, step, k, False)

            @pl.loop(half, chunks)
            def _(k):
                forward(0, step, k, False)
                forward(1, step, k, True)

        if step == far - 2:
            finish_router()

    @pl.loop(0, half)
    def _(k):
        forward(0, far, k, False)
        forward(1, far, k + half, False)

    for distance in range(chips):

        @pl.loop(0, chunks)
        def _(k):
            pair(distance, lax.rem(chip + distance, chips) * 2 + 1 - core, k).wait_recv()

        @pl.loop(0, chunks)
        def _(k):
            pair(distance, shard_of(distance), k).wait_send()

    for step in range(far):
        for way in (0, 1):
            distance = -step if way == 0 else step
            first, last = 0, chunks
            if step == far - 1:
                first, last = (0, half) if way == 0 else (half, chunks)

            @pl.loop(first, last)
            def _(k):
                hop(way, step, shard_of(distance), k).wait_send()

    for peer in peers:
        send_max(peer).wait_send()
        send_part(peer).wait_send()

    @pl.loop(1, banks)
    def _(d):
        column_copy(bank, lax.rem(bank + d, banks)).wait_send()


def put_out(final, scale, router, final_hbm, scale_hbm, router_hbm, sem):
    share = final.shape[0] // PUTS
    copies = [
        pltpu.make_async_copy(
            final.at[pl.ds(i * share, share)], final_hbm.at[pl.ds(i * share, share)], sem.at[i]
        )
        for i in range(PUTS)
    ]
    copies.append(pltpu.make_async_copy(scale, scale_hbm, sem.at[PUTS]))
    copies.append(pltpu.make_async_copy(router, router_hbm, sem.at[PUTS + 1]))
    for copy in copies:
        copy.start()
    for copy in copies:
        copy.wait()


def per_device(banks, zeros, master_down, router_weight, router_gain):
    experts, inner, width = master_down.shape
    total = experts * inner
    chunks, chips = total // CHUNK, zeros // 2
    dma = pltpu.SemaphoreType.DMA
    final, scale, router = pl.pallas_call(
        functools.partial(kernel, banks, zeros),
        out_shape=(
            jax.ShapeDtypeStruct((total, width * zeros), jnp.bfloat16),
            jax.ShapeDtypeStruct((experts, inner), jnp.float32),
            jax.ShapeDtypeStruct((2 * banks, LANES * zeros), jnp.bfloat16),
        ),
        in_specs=[pl.BlockSpec(memory_space=pltpu.HBM)] * 3,
        out_specs=(pl.BlockSpec(memory_space=pltpu.VMEM),) * 3,
        scratch_shapes=[
            pltpu.VMEM((total, LANES), jnp.float32),
            pltpu.VMEM((2, LANES), jnp.float32),
            pltpu.VMEM((1, LANES), jnp.float32),
            pltpu.VMEM((zeros, total // LANES, LANES), jnp.float32),
            pltpu.VMEM((total // LANES, LANES), jnp.float32),
            pltpu.VMEM((zeros, 1, 2 * LANES), jnp.float32),
            pltpu.VMEM((2 * banks * zeros, LANES), jnp.float32),
            dma((LOADS + 2,)),
            dma((zeros,)),
            dma((zeros,)),
            dma((zeros,)),
            dma((zeros,)),
            dma((banks,)),
            dma((banks,)),
            dma((2, chips // 2, chunks)),
            dma((2, chips // 2, chunks)),
            dma((chips, chunks)),
            dma((chips, chunks)),
        ],
        compiler_params=pltpu.CompilerParams(
            collective_id=0, has_side_effects=True, vmem_limit_bytes=24 * 1024 * 1024
        ),
    )(
        *(
            pltpu.with_memory_space_constraint(a, pltpu.HBM)
            for a in (
                master_down.reshape(total, width),
                router_weight.T,
                router_gain.reshape(1, LANES),
            )
        )
    )
    final, scale, router = pl.pallas_call(
        put_out,
        out_shape=tuple(jax.ShapeDtypeStruct(a.shape, a.dtype) for a in (final, scale, router)),
        in_specs=[pl.BlockSpec(memory_space=pltpu.VMEM)] * 3,
        out_specs=(pl.BlockSpec(memory_space=pltpu.HBM),) * 3,
        scratch_shapes=[dma((PUTS + 2,))],
        compiler_params=pltpu.CompilerParams(vmem_limit_bytes=1024 * 1024),
    )(final, scale, router)
    return final.reshape(experts, inner, width * zeros), scale, router.T


def solution(mesh):
    banks, zeros = mesh.shape["bank"], mesh.shape["zero"]
    return jax.shard_map(
        functools.partial(per_device, banks, zeros),
        mesh=mesh,
        in_specs=(P("bank", None, "zero"), P("zero", "bank"), P("zero")),
        out_specs=(P("bank", None, None), P("bank", None), P()),
        check_vma=False,
    )
```

```python
import functools

import jax
import jax.numpy as jnp
from jax import lax
from jax.experimental import pallas as pl
from jax.experimental.pallas import tpu as pltpu
from jax.sharding import PartitionSpec as P

MESH = pl.DeviceIdType.MESH
LANES = 128
ACROSS = 4
CHUNKS = 4
PUTS = 8
ORDER = ((0, 1, 2, 3), (1, 0, 3, 2))
ONWARD = ((0, 2), (1, 3))


def kernel(
    banks, zeros, w_hbm, r_hbm, g_hbm, out, scale, router,
    w, r, g, maxima, rows, parts, columns,
    load_sem, max_send, max_recv, part_send, part_recv, col_send, x_recv, y_recv,
    ring_send, ring_recv, pair_send, pair_recv,
):
    total = w_hbm.shape[0]
    chunk, blocks = total // CHUNKS, total // LANES
    half_blocks = blocks // 2
    chips, down = zeros // 2, banks // ACROSS
    far = chips // 2
    bank, zero = lax.axis_index("bank"), lax.axis_index("zero")
    chip, core = zero // 2, lax.rem(zero, 2)
    partner = chip * 2 + 1 - core
    y, x = bank // ACROSS, lax.rem(bank, ACROSS)

    def shard_of(distance):
        return lax.rem(chip + distance + chips, chips) * 2 + core

    def along_x(distance):
        return y * ACROSS + lax.rem(x + distance + ACROSS, ACROSS)

    def along_y(distance):
        return lax.rem(y + distance + down, down)

    def remote(src, dst, send_sem, recv_sem, **device):
        return pltpu.make_async_remote_copy(
            src_ref=src, dst_ref=dst, send_sem=send_sem, recv_sem=recv_sem,
            device_id=device, device_id_type=MESH,
        )

    offsets = sorted(range(1, chips), key=lambda o: -min(o, chips - o))
    peers = [lax.rem(chip + o, chips) * 2 + c for o in offsets for c in (core, 1 - core)]
    peers.append(partner)
    barrier = pltpu.get_barrier_semaphore()
    for peer in peers:
        pl.semaphore_signal(barrier, inc=1, device_id={"zero": peer}, device_id_type=MESH)

    def load(i):
        at = pl.ds(i * chunk, chunk)
        return pltpu.make_async_copy(w_hbm.at[at], w.at[at], load_sem.at[i])

    load_r = pltpu.make_async_copy(r_hbm, r, load_sem.at[CHUNKS])
    load_g = pltpu.make_async_copy(g_hbm, g, load_sem.at[CHUNKS + 1])
    for i in range(CHUNKS):
        load(i).start()
    load_r.start()
    load_g.start()
    beside = [along_x(1), along_x(-1), along_y(1) * ACROSS + x]
    if down > 2:
        beside.append(along_y(-1) * ACROSS + x)
    for peer in beside:
        pl.semaphore_signal(barrier, inc=1, device_id={"bank": peer}, device_id_type=MESH)

    for i in range(CHUNKS):
        load(i).wait()
        for j in range(i * blocks // CHUNKS, (i + 1) * blocks // CHUNKS):
            block = jnp.abs(w[j * LANES : (j + 1) * LANES, :])
            h, k = j // half_blocks, j % half_blocks
            maxima[h, zero, k : k + 1, :] = jnp.max(block.T, axis=0, keepdims=True)
    load_r.wait()
    load_g.wait()
    product = r[...] * g[...]
    parts[zero, :, 0:LANES] = product[0:1]
    parts[zero, :, LANES : 2 * LANES] = product[1:2]

    pl.semaphore_wait(barrier, zeros - 1 + len(beside))

    for h in (0, 1):
        for peer in peers:
            mine = maxima.at[h, zero]
            remote(mine, mine, max_send.at[h], max_recv.at[h], zero=peer).start()
    for peer in peers:
        mine = parts.at[zero]
        remote(mine, mine, part_send.at[0], part_recv.at[0], zero=peer).start()

    right, left = shard_of(1), shard_of(-1)

    def piece(shard, k):
        return out.at[
            pl.ds(k * chunk, chunk), pl.ds(pl.multiple_of(shard * LANES, LANES), LANES)
        ]

    def hop(way, step, shard, k):
        at = piece(shard, k)
        return remote(
            at, at, ring_send.at[0], ring_recv.at[way, step, k], zero=(right, left)[way]
        )

    def pair(shard, k):
        at = piece(shard, k)
        return remote(at, at, pair_send.at[0], pair_recv.at[0], zero=partner)

    def divide(k):
        for j in range(k * blocks // CHUNKS, (k + 1) * blocks // CHUNKS):
            at = pl.ds(j * LANES, LANES)
            by = jnp.broadcast_to(rows[j : j + 1, :], (LANES, LANES)).T
            to = pl.ds(pl.multiple_of(zero * LANES, LANES), LANES)
            out[at, to] = (w[at, :] / by).astype(jnp.bfloat16)

    for h in (0, 1):
        others = maxima.at[h, pl.ds(0, zeros - 1)]
        remote(others, others, max_send.at[h], max_recv.at[h], zero=partner).wait_recv()
        most = maxima[h, 0]
        for i in range(1, zeros):
            most = jnp.maximum(most, maxima[h, i])
        rows[h * half_blocks : (h + 1) * half_blocks, :] = most
        first, second = 2 * h, 2 * h + 1
        divide(first)
        hop(0, 0, zero, first).start()
        divide(second)
        hop(1, 0, zero, second).start()
        hop(0, 0, zero, second).start()
        hop(1, 0, zero, first).start()
        pair(zero, first).start()
        pair(zero, second).start()

    per_expert = blocks // scale.shape[0]
    for j in range(blocks):
        e, at = j // per_expert, (j % per_expert) * LANES
        scale[e : e + 1, at : at + LANES] = rows[j : j + 1, :]

    def banks_of(first, count):
        size = count * 2 * zeros
        return columns.at[pl.ds(pl.multiple_of(first * 2 * zeros, 2 * zeros), size)]

    def send_x(distance, peer):
        at = banks_of(along_x(distance), 1)
        return remote(at, at, col_send.at[0], x_recv.at[distance % ACROSS], bank=peer)

    def send_y(distance, peer):
        at = banks_of(along_y(distance) * ACROSS, ACROSS)
        return remote(
            at, at, col_send.at[0], y_recv.at[distance % down], bank=peer * ACROSS + x
        )

    def x_first():
        others = parts.at[pl.ds(0, zeros - 1)]
        remote(others, others, part_send.at[0], part_recv.at[0], zero=partner).wait_recv()
        tile = pl.multiple_of(bank * 2 * zeros, 2 * zeros)
        for i in range(zeros):
            columns[pl.ds(tile + i, 1), :] = parts[i, :, 0:LANES]
            columns[pl.ds(tile + zeros + i, 1), :] = parts[i, :, LANES : 2 * LANES]
        at = banks_of(bank, 1)
        remote(at, at, col_send.at[0], x_recv.at[ACROSS - 1], bank=along_x(1)).start()
        remote(at, at, col_send.at[0], x_recv.at[1], bank=along_x(-1)).start()

    def x_second():
        send_x(-1, along_x(1)).wait_recv()
        send_x(1, along_x(-1)).wait_recv()
        at = banks_of(along_x(-1), 1)
        remote(at, at, col_send.at[0], x_recv.at[2], bank=along_x(1)).start()

    ups, downs = down // 2, (down - 1) // 2

    def y_step(step):
        if step == 0:
            send_x(2, along_x(1)).wait_recv()
        if 1 <= step <= ups:
            send_y(-step, along_y(1)).wait_recv()
        if 1 <= step <= downs:
            send_y(step, along_y(-1)).wait_recv()
        if step < ups:
            at = banks_of(along_y(-step) * ACROSS, ACROSS)
            remote(
                at, at, col_send.at[0], y_recv.at[(-step - 1) % down],
                bank=along_y(1) * ACROSS + x,
            ).start()
        if step < downs:
            at = banks_of(along_y(step) * ACROSS, ACROSS)
            remote(
                at, at, col_send.at[0], y_recv.at[(step + 1) % down],
                bank=along_y(-1) * ACROSS + x,
            ).start()

    def finish_router():
        for i in range(zeros):
            router[:, i * LANES : (i + 1) * LANES] = columns[
                pl.ds(i, 2 * banks, stride=zeros), :
            ].astype(jnp.bfloat16)

    stages = [x_second] + [functools.partial(y_step, step) for step in range(ups + 1)]

    def forward(way, step, k, onward):
        shard = shard_of(-step if way == 0 else step)
        hop(way, step - 1, shard, k).wait_recv()
        if onward:
            hop(way, step, shard, k).start()
        pair(shard, k).start()

    x_first()
    for step in range(1, far):
        for i in range(CHUNKS):
            for way in (0, 1):
                k = ORDER[way][i]
                forward(way, step, k, step < far - 1 or k in ONWARD[way])
            if i % 2 == 1 and stages:
                stages.pop(0)()
    for stage in stages:
        stage()
    finish_router()
    for i in range(CHUNKS // 2):
        for way in (0, 1):
            forward(way, far, ONWARD[way][i], False)

    sent = out.at[:, pl.ds(0, (chips - 1) * LANES)]
    remote(sent, sent, ring_send.at[0], ring_recv.at[0, 0, 0], zero=right).wait_send()
    for h in (0, 1):
        others = maxima.at[h, pl.ds(0, zeros - 1)]
        remote(others, others, max_send.at[h], max_recv.at[h], zero=partner).wait_send()
    others = parts.at[pl.ds(0, zeros - 1)]
    remote(others, others, part_send.at[0], part_recv.at[0], zero=partner).wait_send()
    size = (ACROSS - 1 + (down - 1) * ACROSS) * 2 * zeros
    others = columns.at[pl.ds(0, size)]
    remote(others, others, col_send.at[0], x_recv.at[0], bank=along_x(1)).wait_send()
    both = out.at[:, pl.ds(0, chips * LANES)]
    remote(both, both, pair_send.at[0], pair_recv.at[0], zero=partner).wait()


def put_out(final, scale, router, final_hbm, scale_hbm, router_hbm, sem):
    share = final.shape[0] // PUTS
    copies = [
        pltpu.make_async_copy(
            final.at[pl.ds(i * share, share)], final_hbm.at[pl.ds(i * share, share)], sem.at[i]
        )
        for i in range(PUTS)
    ]
    copies.append(pltpu.make_async_copy(scale, scale_hbm, sem.at[PUTS]))
    copies.append(pltpu.make_async_copy(router, router_hbm, sem.at[PUTS + 1]))
    for copy in copies:
        copy.start()
    for copy in copies:
        copy.wait()


def per_device(banks, zeros, master_down, router_weight, router_gain):
    experts, inner, width = master_down.shape
    total = experts * inner
    chips = zeros // 2
    dma = pltpu.SemaphoreType.DMA
    final, scale, router = pl.pallas_call(
        functools.partial(kernel, banks, zeros),
        out_shape=(
            jax.ShapeDtypeStruct((total, width * zeros), jnp.bfloat16),
            jax.ShapeDtypeStruct((experts, inner), jnp.float32),
            jax.ShapeDtypeStruct((2 * banks, LANES * zeros), jnp.bfloat16),
        ),
        in_specs=[pl.BlockSpec(memory_space=pltpu.HBM)] * 3,
        out_specs=(pl.BlockSpec(memory_space=pltpu.VMEM),) * 3,
        scratch_shapes=[
            pltpu.VMEM((total, LANES), jnp.float32),
            pltpu.VMEM((2, LANES), jnp.float32),
            pltpu.VMEM((1, LANES), jnp.float32),
            pltpu.VMEM((2, zeros, total // LANES // 2, LANES), jnp.float32),
            pltpu.VMEM((total // LANES, LANES), jnp.float32),
            pltpu.VMEM((zeros, 1, 2 * LANES), jnp.float32),
            pltpu.VMEM((2 * banks * zeros, LANES), jnp.float32),
            dma((CHUNKS + 2,)),
            dma((2,)),
            dma((2,)),
            dma((1,)),
            dma((1,)),
            dma((1,)),
            dma((ACROSS,)),
            dma((banks // ACROSS,)),
            dma((1,)),
            dma((2, chips // 2, CHUNKS)),
            dma((1,)),
            dma((1,)),
        ],
        compiler_params=pltpu.CompilerParams(
            collective_id=0, has_side_effects=True, vmem_limit_bytes=24 * 1024 * 1024
        ),
    )(
        *(
            pltpu.with_memory_space_constraint(a, pltpu.HBM)
            for a in (
                master_down.reshape(total, width),
                router_weight.T,
                router_gain.reshape(1, LANES),
            )
        )
    )
    final, scale, router = pl.pallas_call(
        put_out,
        out_shape=tuple(jax.ShapeDtypeStruct(a.shape, a.dtype) for a in (final, scale, router)),
        in_specs=[pl.BlockSpec(memory_space=pltpu.VMEM)] * 3,
        out_specs=(pl.BlockSpec(memory_space=pltpu.HBM),) * 3,
        scratch_shapes=[dma((PUTS + 2,))],
        compiler_params=pltpu.CompilerParams(vmem_limit_bytes=1024 * 1024),
    )(final, scale, router)
    return final.reshape(experts, inner, width * zeros), scale, router.T


def solution(mesh):
    banks, zeros = mesh.shape["bank"], mesh.shape["zero"]
    return jax.shard_map(
        functools.partial(per_device, banks, zeros),
        mesh=mesh,
        in_specs=(P("bank", None, "zero"), P("zero", "bank"), P("zero")),
        out_specs=(P("bank", None, None), P("bank", None), P()),
        check_vma=False,
    )
```

```python
import functools

import jax
import jax.numpy as jnp
from jax import lax
from jax.experimental import pallas as pl
from jax.experimental.pallas import tpu as pltpu
from jax.sharding import PartitionSpec as P

MESH = pl.DeviceIdType.MESH
LANES = 128
ACROSS = 4
LOADS = 4
PUTS = 8
PIECES = (4, 2, 2, 4, 4)
EARLY = PIECES[0] * LANES
ORDER = ((0, 1, 2, 3, 4), (0, 1, 3, 4, 2))
ONWARD = ((0, 1, 2), (3, 4))


def arrivals(chips):
    keys = [
        (way, step, k)
        for way in (0, 1)
        for step in range(chips // 2)
        for k in range(len(PIECES))
        if step < chips // 2 - 1 or k in ONWARD[way]
    ]
    return {key: i for i, key in enumerate(keys)}


def kernel(
    banks, zeros, w_hbm, r_hbm, g_hbm, out, scale, router,
    w, r, g, early, maxima, shared, rows, parts, columns,
    load_sem, max_send, max_recv, part_send, part_recv, col_send, x_recv, y_recv,
    early_send, ring_send, ring_recv, pair_send, pair_recv,
):
    total = w_hbm.shape[0]
    blocks = total // LANES
    half_blocks = blocks // 2
    chips, down = zeros // 2, banks // ACROSS
    far, number = chips // 2, arrivals(chips)
    bank, zero = lax.axis_index("bank"), lax.axis_index("zero")
    chip, core = zero // 2, lax.rem(zero, 2)
    partner = chip * 2 + 1 - core
    y, x = bank // ACROSS, lax.rem(bank, ACROSS)

    def shard_of(distance):
        return lax.rem(chip + distance + chips, chips) * 2 + core

    def along_x(distance):
        return y * ACROSS + lax.rem(x + distance + ACROSS, ACROSS)

    def along_y(distance):
        return lax.rem(y + distance + down, down)

    def remote(src, dst, send_sem, recv_sem, **device):
        return pltpu.make_async_remote_copy(
            src_ref=src, dst_ref=dst, send_sem=send_sem, recv_sem=recv_sem,
            device_id=device, device_id_type=MESH,
        )

    offsets = sorted(range(1, chips), key=lambda o: -min(o, chips - o))
    peers = [lax.rem(chip + o, chips) * 2 + c for o in offsets for c in (core, 1 - core)]
    peers.append(partner)
    barrier = pltpu.get_barrier_semaphore()
    for peer in peers:
        pl.semaphore_signal(barrier, inc=1, device_id={"zero": peer}, device_id_type=MESH)

    share = total // LOADS

    def load(i):
        at = pl.ds(i * share, share)
        return pltpu.make_async_copy(w_hbm.at[at], w.at[at], load_sem.at[i])

    load_r = pltpu.make_async_copy(r_hbm, r, load_sem.at[LOADS])
    load_g = pltpu.make_async_copy(g_hbm, g, load_sem.at[LOADS + 1])
    for i in range(LOADS):
        load(i).start()
    load_r.start()
    load_g.start()
    beside = [along_x(1), along_x(-1), along_y(1) * ACROSS + x]
    if down > 2:
        beside.append(along_y(-1) * ACROSS + x)
    for peer in beside:
        pl.semaphore_signal(barrier, inc=1, device_id={"bank": peer}, device_id_type=MESH)

    for i in range(LOADS):
        load(i).wait()
        for j in range(i * blocks // LOADS, (i + 1) * blocks // LOADS):
            block = jnp.abs(w[j * LANES : (j + 1) * LANES, :])
            h, k = j // half_blocks, j % half_blocks
            maxima[h, zero, k : k + 1, :] = jnp.max(block.T, axis=0, keepdims=True)
    load_r.wait()
    load_g.wait()
    product = r[...] * g[...]
    parts[zero, :, 0:LANES] = product[0:1]
    parts[zero, :, LANES : 2 * LANES] = product[1:2]

    pl.semaphore_wait(barrier, zeros - 1 + len(beside))

    mine = maxima.at[0, zero]
    for peer in peers:
        remote(mine, mine, max_send.at[0], max_recv.at[0], zero=peer).start()
    mine = maxima.at[1, zero]
    for peer in peers[0:-1:2]:
        remote(mine, mine, max_send.at[1], max_recv.at[1], zero=peer).start()

    right, left = shard_of(1), shard_of(-1)
    starts = [sum(PIECES[:k]) for k in range(len(PIECES) + 1)]

    def first_rows(way):
        return remote(
            w.at[pl.ds(0, EARLY)], early.at[way], early_send.at[0],
            ring_recv.at[number[way, 0, 0]], zero=(right, left)[way],
        )

    @pl.when(core == 0)
    def _():
        first_rows(0).start()
        first_rows(1).start()

    for peer in peers:
        mine = parts.at[zero]
        remote(mine, mine, part_send.at[0], part_recv.at[0], zero=peer).start()

    def piece(shard, k):
        return out.at[
            pl.ds(starts[k] * LANES, PIECES[k] * LANES),
            pl.ds(pl.multiple_of(shard * LANES, LANES), LANES),
        ]

    def hop(way, step, shard, k):
        at = piece(shard, k)
        sem = early_send if step == 0 and k == 0 else ring_send
        return remote(
            at, at, sem.at[0], ring_recv.at[number[way, step, k]], zero=(right, left)[way]
        )

    def pair(shard, k):
        at = piece(shard, k)
        return remote(at, at, pair_send.at[0], pair_recv.at[0], zero=partner)

    def divide(k, shard=zero, source=w):
        for j in range(starts[k], starts[k + 1]):
            at = pl.ds(j * LANES, LANES)
            by = jnp.broadcast_to(rows[j : j + 1, :], (LANES, LANES)).T
            to = pl.ds(pl.multiple_of(shard * LANES, LANES), LANES)
            out[at, to] = (source[at, :] / by).astype(jnp.bfloat16)

    others = maxima.at[0, pl.ds(0, zeros - 1)]
    remote(others, others, max_send.at[0], max_recv.at[0], zero=partner).wait_recv()
    most = maxima[0, 0]
    for i in range(1, zeros):
        most = jnp.maximum(most, maxima[0, i])
    rows[0:half_blocks, :] = most

    @pl.when(core == 1)
    def _():
        divide(0)
        hop(0, 0, zero, 0).start()
        hop(1, 0, zero, 0).start()

    divide(1)
    hop(0, 0, zero, 1).start()
    hop(1, 0, zero, 1).start()
    divide(2)
    hop(0, 0, zero, 2).start()

    others = maxima.at[1, pl.ds(0, chips - 1)]
    remote(others, others, max_send.at[1], max_recv.at[1], zero=partner).wait_recv()
    most = maxima[1, core]
    for i in range(1, chips):
        most = jnp.maximum(most, maxima[1, 2 * i + core])
    shared[core] = most
    ours = shared.at[core]
    share_max = remote(ours, ours, pair_send.at[1], pair_recv.at[1], zero=partner)
    share_max.start()

    @pl.when(core == 0)
    def _():
        divide(0)

    for k in (0, 1, 2):
        pair(zero, k).start()
    share_max.wait_recv()
    rows[half_blocks:blocks, :] = jnp.maximum(shared[0], shared[1])
    divide(3)
    hop(0, 0, zero, 3).start()
    hop(1, 0, zero, 3).start()
    divide(4)
    hop(0, 0, zero, 4).start()
    hop(1, 0, zero, 4).start()
    hop(1, 0, zero, 2).start()
    for k in (3, 4):
        pair(zero, k).start()

    per_expert = blocks // scale.shape[0]
    for j in range(blocks):
        e, at = j // per_expert, (j % per_expert) * LANES
        scale[e : e + 1, at : at + LANES] = rows[j : j + 1, :]

    def banks_of(first, count):
        size = count * 2 * zeros
        return columns.at[pl.ds(pl.multiple_of(first * 2 * zeros, 2 * zeros), size)]

    def send_x(distance, peer):
        at = banks_of(along_x(distance), 1)
        return remote(at, at, col_send.at[0], x_recv.at[distance % ACROSS], bank=peer)

    def send_y(distance, peer):
        at = banks_of(along_y(distance) * ACROSS, ACROSS)
        return remote(
            at, at, col_send.at[0], y_recv.at[distance % down], bank=peer * ACROSS + x
        )

    def x_first():
        others = parts.at[pl.ds(0, zeros - 1)]
        remote(others, others, part_send.at[0], part_recv.at[0], zero=partner).wait_recv()
        tile = pl.multiple_of(bank * 2 * zeros, 2 * zeros)
        for i in range(zeros):
            columns[pl.ds(tile + i, 1), :] = parts[i, :, 0:LANES]
            columns[pl.ds(tile + zeros + i, 1), :] = parts[i, :, LANES : 2 * LANES]
        at = banks_of(bank, 1)
        remote(at, at, col_send.at[0], x_recv.at[ACROSS - 1], bank=along_x(1)).start()
        remote(at, at, col_send.at[0], x_recv.at[1], bank=along_x(-1)).start()

    def x_second():
        send_x(-1, along_x(1)).wait_recv()
        send_x(1, along_x(-1)).wait_recv()
        at = banks_of(along_x(-1), 1)
        remote(at, at, col_send.at[0], x_recv.at[2], bank=along_x(1)).start()

    ups, downs = down // 2, (down - 1) // 2

    def y_step(step):
        if step == 0:
            send_x(2, along_x(1)).wait_recv()
        if 1 <= step <= ups:
            send_y(-step, along_y(1)).wait_recv()
        if 1 <= step <= downs:
            send_y(step, along_y(-1)).wait_recv()
        if step < ups:
            at = banks_of(along_y(-step) * ACROSS, ACROSS)
            remote(
                at, at, col_send.at[0], y_recv.at[(-step - 1) % down],
                bank=along_y(1) * ACROSS + x,
            ).start()
        if step < downs:
            at = banks_of(along_y(step) * ACROSS, ACROSS)
            remote(
                at, at, col_send.at[0], y_recv.at[(step + 1) % down],
                bank=along_y(-1) * ACROSS + x,
            ).start()

    def finish_router():
        for i in range(zeros):
            router[:, i * LANES : (i + 1) * LANES] = columns[
                pl.ds(i, 2 * banks, stride=zeros), :
            ].astype(jnp.bfloat16)

    stages = [x_first, x_second] + [functools.partial(y_step, step) for step in range(ups + 1)]

    def forward(way, step, k, onward):
        shard = shard_of(-step if way == 0 else step)
        if step == 1 and k == 0:

            @pl.when(core == 0)
            def _():
                first_rows(way).wait_recv()
                divide(0, shard, early.at[way])

            @pl.when(core == 1)
            def _():
                hop(way, 0, shard, 0).wait_recv()
        else:
            hop(way, step - 1, shard, k).wait_recv()
        if onward:
            hop(way, step, shard, k).start()
        pair(shard, k).start()

    turn = 0
    for step in range(1, far):
        for i in range(len(PIECES)):
            for way in (0, 1):
                k = ORDER[way][i]
                forward(way, step, k, step < far - 1 or k in ONWARD[way])
            if turn % 2 == 1 and stages:
                stages.pop(0)()
            turn += 1
    for stage in stages:
        stage()
    finish_router()
    for i in range(len(PIECES)):
        for way in (0, 1):
            if ORDER[way][i] in ONWARD[way]:
                forward(way, far, ORDER[way][i], False)

    size = (blocks * (chips - 1) - 2 * PIECES[0]) * LANES // chips
    sent = out.at[pl.ds(0, size), pl.ds(0, chips * LANES)]
    remote(sent, sent, ring_send.at[0], pair_recv.at[0], zero=right).wait_send()

    @pl.when(core == 0)
    def _():
        remote(early, early, early_send.at[0], pair_recv.at[0], zero=right).wait_send()

    @pl.when(core == 1)
    def _():
        sent = out.at[pl.ds(0, 2 * EARLY), pl.ds(0, LANES)]
        remote(sent, sent, early_send.at[0], pair_recv.at[0], zero=right).wait_send()

    for h, count in ((0, zeros - 1), (1, chips - 1)):
        others = maxima.at[h, pl.ds(0, count)]
        remote(others, others, max_send.at[h], max_recv.at[h], zero=partner).wait_send()
    share_max.wait_send()
    others = parts.at[pl.ds(0, zeros - 1)]
    remote(others, others, part_send.at[0], part_recv.at[0], zero=partner).wait_send()
    size = (ACROSS - 1 + (down - 1) * ACROSS) * 2 * zeros
    others = columns.at[pl.ds(0, size)]
    remote(others, others, col_send.at[0], x_recv.at[0], bank=along_x(1)).wait_send()
    both = out.at[:, pl.ds(0, chips * LANES)]
    remote(both, both, pair_send.at[0], pair_recv.at[0], zero=partner).wait()


def put_out(final, scale, router, final_hbm, scale_hbm, router_hbm, sem):
    share = final.shape[0] // PUTS
    copies = [
        pltpu.make_async_copy(
            final.at[pl.ds(i * share, share)], final_hbm.at[pl.ds(i * share, share)], sem.at[i]
        )
        for i in range(PUTS)
    ]
    copies.append(pltpu.make_async_copy(scale, scale_hbm, sem.at[PUTS]))
    copies.append(pltpu.make_async_copy(router, router_hbm, sem.at[PUTS + 1]))
    for copy in copies:
        copy.start()
    for copy in copies:
        copy.wait()


def per_device(banks, zeros, master_down, router_weight, router_gain):
    experts, inner, width = master_down.shape
    total = experts * inner
    chips = zeros // 2
    dma = pltpu.SemaphoreType.DMA
    final, scale, router = pl.pallas_call(
        functools.partial(kernel, banks, zeros),
        out_shape=(
            jax.ShapeDtypeStruct((total, width * zeros), jnp.bfloat16),
            jax.ShapeDtypeStruct((experts, inner), jnp.float32),
            jax.ShapeDtypeStruct((2 * banks, LANES * zeros), jnp.bfloat16),
        ),
        in_specs=[pl.BlockSpec(memory_space=pltpu.HBM)] * 3,
        out_specs=(pl.BlockSpec(memory_space=pltpu.VMEM),) * 3,
        scratch_shapes=[
            pltpu.VMEM((total, LANES), jnp.float32),
            pltpu.VMEM((2, LANES), jnp.float32),
            pltpu.VMEM((1, LANES), jnp.float32),
            pltpu.VMEM((2, EARLY, LANES), jnp.float32),
            pltpu.VMEM((2, zeros, total // LANES // 2, LANES), jnp.float32),
            pltpu.VMEM((2, total // LANES // 2, LANES), jnp.float32),
            pltpu.VMEM((total // LANES, LANES), jnp.float32),
            pltpu.VMEM((zeros, 1, 2 * LANES), jnp.float32),
            pltpu.VMEM((2 * banks * zeros, LANES), jnp.float32),
            dma((LOADS + 2,)),
            dma((2,)),
            dma((2,)),
            dma((1,)),
            dma((1,)),
            dma((1,)),
            dma((ACROSS,)),
            dma((banks // ACROSS,)),
            dma((1,)),
            dma((1,)),
            dma((len(arrivals(chips)),)),
            dma((2,)),
            dma((2,)),
        ],
        compiler_params=pltpu.CompilerParams(
            collective_id=0, has_side_effects=True, vmem_limit_bytes=24 * 1024 * 1024
        ),
    )(
        *(
            pltpu.with_memory_space_constraint(a, pltpu.HBM)
            for a in (
                master_down.reshape(total, width),
                router_weight.T,
                router_gain.reshape(1, LANES),
            )
        )
    )
    final, scale, router = pl.pallas_call(
        put_out,
        out_shape=tuple(jax.ShapeDtypeStruct(a.shape, a.dtype) for a in (final, scale, router)),
        in_specs=[pl.BlockSpec(memory_space=pltpu.VMEM)] * 3,
        out_specs=(pl.BlockSpec(memory_space=pltpu.HBM),) * 3,
        scratch_shapes=[dma((PUTS + 2,))],
        compiler_params=pltpu.CompilerParams(vmem_limit_bytes=1024 * 1024),
    )(final, scale, router)
    return final.reshape(experts, inner, width * zeros), scale, router.T


def solution(mesh):
    banks, zeros = mesh.shape["bank"], mesh.shape["zero"]
    return jax.shard_map(
        functools.partial(per_device, banks, zeros),
        mesh=mesh,
        in_specs=(P("bank", None, "zero"), P("zero", "bank"), P("zero")),
        out_specs=(P("bank", None, None), P("bank", None), P()),
        check_vma=False,
    )
```

```python
import functools

import jax
import jax.numpy as jnp
from jax import lax
from jax.experimental import pallas as pl
from jax.experimental.pallas import tpu as pltpu
from jax.sharding import PartitionSpec as P

MESH = pl.DeviceIdType.MESH
LANES = 128
ACROSS = 4
LOADS = 4
PUTS = 8
PIECES = (4, 4, 6, 2)
AHEAD = 2
EARLY = PIECES[AHEAD] * LANES
ORDER = ((0, 1, 2, 3), (0, 2, 3, 1))
ONWARD = ((0, 1), (2, 3))
TURNS = (0, 2, 4, 5, 7, 8, 10)


def arrivals(chips):
    keys = [
        (way, step, k)
        for way in (0, 1)
        for step in range(chips // 2)
        for k in range(len(PIECES))
        if step < chips // 2 - 1 or k in ONWARD[way]
    ]
    return {key: i for i, key in enumerate(keys)}


def kernel(
    banks, zeros, w_hbm, r_hbm, g_hbm, out, scale, router,
    w, r, g, early, maxima, shared, rows, parts, columns,
    load_sem, max_send, max_recv, part_send, part_recv, col_send, x_recv, y_recv,
    early_send, ring_send, ring_recv, pair_send, pair_recv, hello,
):
    total = w_hbm.shape[0]
    blocks = total // LANES
    half_blocks = blocks // 2
    chips, down = zeros // 2, banks // ACROSS
    far, number = chips // 2, arrivals(chips)
    bank, zero = lax.axis_index("bank"), lax.axis_index("zero")
    chip, core = zero // 2, lax.rem(zero, 2)
    partner = chip * 2 + 1 - core
    y, x = bank // ACROSS, lax.rem(bank, ACROSS)

    def shard_of(distance):
        return lax.rem(chip + distance + chips, chips) * 2 + core

    def along_x(distance):
        return y * ACROSS + lax.rem(x + distance + ACROSS, ACROSS)

    def along_y(distance):
        return lax.rem(y + distance + down, down)

    def remote(src, dst, send_sem, recv_sem, **device):
        return pltpu.make_async_remote_copy(
            src_ref=src, dst_ref=dst, send_sem=send_sem, recv_sem=recv_sem,
            device_id=device, device_id_type=MESH,
        )

    offsets = sorted(range(1, chips), key=lambda o: -min(o, chips - o))
    peers = [lax.rem(chip + o, chips) * 2 + c for o in offsets for c in (core, 1 - core)]
    peers.append(partner)
    barrier = pltpu.get_barrier_semaphore()
    for peer in peers:
        pl.semaphore_signal(barrier, inc=1, device_id={"zero": peer}, device_id_type=MESH)

    share = total // LOADS

    def load(i):
        at = pl.ds(i * share, share)
        return pltpu.make_async_copy(w_hbm.at[at], w.at[at], load_sem.at[i])

    load_r = pltpu.make_async_copy(r_hbm, r, load_sem.at[LOADS])
    load_g = pltpu.make_async_copy(g_hbm, g, load_sem.at[LOADS + 1])
    for i in range(LOADS):
        load(i).start()
    load_r.start()
    load_g.start()

    sides = (
        (x, ACROSS, lambda to: to + y * ACROSS, hello.at[0]),
        (y, down, lambda to: to * ACROSS + x, hello.at[1]),
    )

    def to_higher(here, size, bank_of, signal):
        @pl.when(here < size - 1)
        def _():
            signal(bank_of(here + 1))

        if size > 2:

            @pl.when(here == 0)
            def _():
                signal(bank_of(size - 1))

    def to_lower(here, size, bank_of, signal):
        @pl.when(here > 0)
        def _():
            signal(bank_of(here - 1))

        if size > 2:

            @pl.when(here == size - 1)
            def _():
                signal(bank_of(0))

    def lower(here, size):
        return (here + size - 1) // size + ((here + 1) // size if size > 2 else 0)

    def higher(here, size):
        return (2 if size > 2 else 1) - lower(here, size)

    def answers(here, size, sem):
        @pl.when(higher(here, size) > 0)
        def _():
            pl.semaphore_wait(sem, higher(here, size))

    for here, size, bank_of, _ in sides:
        to_higher(
            here, size, bank_of,
            lambda to: pl.semaphore_signal(
                barrier, inc=1, device_id={"bank": to}, device_id_type=MESH
            ),
        )

    for i in range(LOADS):
        load(i).wait()
        for j in range(i * blocks // LOADS, (i + 1) * blocks // LOADS):
            block = jnp.abs(w[j * LANES : (j + 1) * LANES, :])
            h, k = j // half_blocks, j % half_blocks
            maxima[h, zero, k : k + 1, :] = jnp.max(block.T, axis=0, keepdims=True)
    load_r.wait()
    load_g.wait()
    product = r[...] * g[...]
    parts[zero, :, 0:LANES] = product[0:1]
    parts[zero, :, LANES : 2 * LANES] = product[1:2]

    pl.semaphore_wait(barrier, zeros - 1 + lower(x, ACROSS) + lower(y, down))

    mine = maxima.at[0, zero]
    for peer in peers:
        remote(mine, mine, max_send.at[0], max_recv.at[0], zero=peer).start()
    mine = maxima.at[1, zero]
    for peer in peers[0:-1:2]:
        remote(mine, mine, max_send.at[1], max_recv.at[1], zero=peer).start()

    right, left = shard_of(1), shard_of(-1)
    starts = [sum(PIECES[:k]) for k in range(len(PIECES) + 1)]

    def first_rows(way):
        return remote(
            w.at[pl.ds(starts[AHEAD] * LANES, EARLY)], early.at[way], early_send.at[0],
            ring_recv.at[number[way, 0, AHEAD]], zero=(right, left)[way],
        )

    @pl.when(core == 0)
    def _():
        first_rows(0).start()
        first_rows(1).start()

    for peer in peers:
        mine = parts.at[zero]
        remote(mine, mine, part_send.at[0], part_recv.at[0], zero=peer).start()
    for here, size, bank_of, sem in sides:
        to_lower(
            here, size, bank_of,
            lambda to: pl.semaphore_signal(
                sem, inc=1, device_id={"bank": to}, device_id_type=MESH
            ),
        )

    def piece(shard, k):
        return out.at[
            pl.ds(starts[k] * LANES, PIECES[k] * LANES),
            pl.ds(pl.multiple_of(shard * LANES, LANES), LANES),
        ]

    def hop(way, step, shard, k):
        at = piece(shard, k)
        sem = early_send if step == 0 and k == AHEAD else ring_send
        return remote(
            at, at, sem.at[0], ring_recv.at[number[way, step, k]], zero=(right, left)[way]
        )

    def pair(shard, k):
        at = piece(shard, k)
        return remote(at, at, pair_send.at[0], pair_recv.at[0], zero=partner)

    def divide(k, shard=zero, source=w, first=0):
        for j in range(starts[k], starts[k + 1]):
            at, source_at = pl.ds(j * LANES, LANES), pl.ds((j - first) * LANES, LANES)
            by = jnp.broadcast_to(rows[j : j + 1, :], (LANES, LANES)).T
            to = pl.ds(pl.multiple_of(shard * LANES, LANES), LANES)
            out[at, to] = (source[source_at, :] / by).astype(jnp.bfloat16)

    others = maxima.at[0, pl.ds(0, zeros - 1)]
    remote(others, others, max_send.at[0], max_recv.at[0], zero=partner).wait_recv()
    most = maxima[0, 0]
    for i in range(1, zeros):
        most = jnp.maximum(most, maxima[0, i])
    rows[0:half_blocks, :] = most

    divide(0)
    hop(0, 0, zero, 0).start()
    hop(1, 0, zero, 0).start()
    divide(1)
    hop(0, 0, zero, 1).start()

    others = maxima.at[1, pl.ds(0, chips - 1)]
    remote(others, others, max_send.at[1], max_recv.at[1], zero=partner).wait_recv()
    most = maxima[1, core]
    for i in range(1, chips):
        most = jnp.maximum(most, maxima[1, 2 * i + core])
    shared[core] = most
    ours = shared.at[core]
    share_max = remote(ours, ours, pair_send.at[1], pair_recv.at[1], zero=partner)
    share_max.start()

    share_max.wait_recv()
    rows[half_blocks:blocks, :] = jnp.maximum(shared[0], shared[1])
    divide(AHEAD)

    @pl.when(core == 1)
    def _():
        hop(1, 0, zero, AHEAD).start()
        hop(0, 0, zero, AHEAD).start()

    divide(3)
    hop(1, 0, zero, 3).start()
    hop(0, 0, zero, 3).start()
    hop(1, 0, zero, 1).start()
    for k in range(len(PIECES)):
        pair(zero, k).start()

    per_expert = blocks // scale.shape[0]
    for j in range(blocks):
        e, at = j // per_expert, (j % per_expert) * LANES
        scale[e : e + 1, at : at + LANES] = rows[j : j + 1, :]

    def banks_of(first, count):
        size = count * 2 * zeros
        return columns.at[pl.ds(pl.multiple_of(first * 2 * zeros, 2 * zeros), size)]

    def send_x(distance, peer):
        at = banks_of(along_x(distance), 1)
        return remote(at, at, col_send.at[0], x_recv.at[abs(distance) - 1], bank=peer)

    def x_first():
        others = parts.at[pl.ds(0, zeros - 1)]
        remote(others, others, part_send.at[0], part_recv.at[0], zero=partner).wait_recv()
        tile = pl.multiple_of(bank * 2 * zeros, 2 * zeros)
        for i in range(zeros):
            columns[pl.ds(tile + i, 1), :] = parts[i, :, 0:LANES]
            columns[pl.ds(tile + zeros + i, 1), :] = parts[i, :, LANES : 2 * LANES]
        answers(x, ACROSS, hello.at[0])
        at = banks_of(bank, 1)
        remote(at, at, col_send.at[0], x_recv.at[0], bank=along_x(1)).start()
        remote(at, at, col_send.at[0], x_recv.at[0], bank=along_x(-1)).start()

    def x_second():
        both = banks_of(0, 2)
        remote(both, both, col_send.at[0], x_recv.at[0], bank=along_x(1)).wait_recv()
        at = banks_of(along_x(-1), 1)
        remote(at, at, col_send.at[0], x_recv.at[1], bank=along_x(1)).start()

    ups, downs = down // 2, (down - 1) // 2

    def y_step(step):
        if step == 0:
            send_x(2, along_x(1)).wait_recv()
            answers(y, down, hello.at[1])
        if 1 <= step <= ups:
            came = banks_of(0, (2 if step <= downs else 1) * ACROSS)
            remote(
                came, came, col_send.at[0], y_recv.at[step - 1], bank=along_x(1)
            ).wait_recv()
        if step < ups:
            at = banks_of(along_y(-step) * ACROSS, ACROSS)
            remote(
                at, at, col_send.at[0], y_recv.at[step],
                bank=along_y(1) * ACROSS + x,
            ).start()
        if step < downs:
            at = banks_of(along_y(step) * ACROSS, ACROSS)
            remote(
                at, at, col_send.at[0], y_recv.at[step],
                bank=along_y(-1) * ACROSS + x,
            ).start()

    def finish_router():
        for i in range(zeros):
            router[:, i * LANES : (i + 1) * LANES] = columns[
                pl.ds(i, 2 * banks, stride=zeros), :
            ].astype(jnp.bfloat16)

    stages = [x_first, x_second] + [functools.partial(y_step, step) for step in range(ups + 1)]

    def forward(way, step, k, onward):
        shard = shard_of(-step if way == 0 else step)
        if step == 1 and k == AHEAD:

            @pl.when(core == 0)
            def _():
                first_rows(way).wait_recv()
                divide(k, shard, early.at[way], starts[k])

            @pl.when(core == 1)
            def _():
                hop(way, 0, shard, k).wait_recv()
        else:
            hop(way, step - 1, shard, k).wait_recv()
        if onward:
            hop(way, step, shard, k).start()
        pair(shard, k).start()

    turn = 0
    for step in range(1, far):
        for i in range(len(PIECES)):
            for way in (0, 1):
                k = ORDER[way][i]
                forward(way, step, k, step < far - 1 or k in ONWARD[way])
            if turn in TURNS and stages:
                stages.pop(0)()
            turn += 1
    for stage in stages:
        stage()
    finish_router()
    for i in range(len(ONWARD[0])):
        for way in (0, 1):
            forward(way, far, ONWARD[way][i], False)

    size = ((chips - 1) * total - 2 * EARLY) // chips
    sent = out.at[pl.ds(0, size), pl.ds(0, chips * LANES)]
    remote(sent, sent, ring_send.at[0], pair_recv.at[0], zero=right).wait_send()

    @pl.when(core == 0)
    def _():
        remote(early, early, early_send.at[0], pair_recv.at[0], zero=right).wait_send()

    @pl.when(core == 1)
    def _():
        sent = out.at[pl.ds(0, 2 * EARLY), pl.ds(0, LANES)]
        remote(sent, sent, early_send.at[0], pair_recv.at[0], zero=right).wait_send()

    for h, count in ((0, zeros - 1), (1, chips - 1)):
        others = maxima.at[h, pl.ds(0, count)]
        remote(others, others, max_send.at[h], max_recv.at[h], zero=partner).wait_send()
    share_max.wait_send()
    others = parts.at[pl.ds(0, zeros - 1)]
    remote(others, others, part_send.at[0], part_recv.at[0], zero=partner).wait_send()
    size = (ACROSS - 1 + (down - 1) * ACROSS) * 2 * zeros
    others = columns.at[pl.ds(0, size)]
    remote(others, others, col_send.at[0], x_recv.at[0], bank=along_x(1)).wait_send()
    both = out.at[:, pl.ds(0, chips * LANES)]
    remote(both, both, pair_send.at[0], pair_recv.at[0], zero=partner).wait()


def put_out(final, scale, router, final_hbm, scale_hbm, router_hbm, sem):
    share = final.shape[0] // PUTS
    copies = [
        pltpu.make_async_copy(
            final.at[pl.ds(i * share, share)], final_hbm.at[pl.ds(i * share, share)], sem.at[i]
        )
        for i in range(PUTS)
    ]
    copies.append(pltpu.make_async_copy(scale, scale_hbm, sem.at[PUTS]))
    copies.append(pltpu.make_async_copy(router, router_hbm, sem.at[PUTS + 1]))
    for copy in copies:
        copy.start()
    for copy in copies:
        copy.wait()


def per_device(banks, zeros, master_down, router_weight, router_gain):
    experts, inner, width = master_down.shape
    total = experts * inner
    chips = zeros // 2
    dma = pltpu.SemaphoreType.DMA
    final, scale, router = pl.pallas_call(
        functools.partial(kernel, banks, zeros),
        out_shape=(
            jax.ShapeDtypeStruct((total, width * zeros), jnp.bfloat16),
            jax.ShapeDtypeStruct((experts, inner), jnp.float32),
            jax.ShapeDtypeStruct((2 * banks, LANES * zeros), jnp.bfloat16),
        ),
        in_specs=[pl.BlockSpec(memory_space=pltpu.HBM)] * 3,
        out_specs=(pl.BlockSpec(memory_space=pltpu.VMEM),) * 3,
        scratch_shapes=[
            pltpu.VMEM((total, LANES), jnp.float32),
            pltpu.VMEM((2, LANES), jnp.float32),
            pltpu.VMEM((1, LANES), jnp.float32),
            pltpu.VMEM((2, EARLY, LANES), jnp.float32),
            pltpu.VMEM((2, zeros, total // LANES // 2, LANES), jnp.float32),
            pltpu.VMEM((2, total // LANES // 2, LANES), jnp.float32),
            pltpu.VMEM((total // LANES, LANES), jnp.float32),
            pltpu.VMEM((zeros, 1, 2 * LANES), jnp.float32),
            pltpu.VMEM((2 * banks * zeros, LANES), jnp.float32),
            dma((LOADS + 2,)),
            dma((2,)),
            dma((2,)),
            dma((1,)),
            dma((1,)),
            dma((1,)),
            dma((ACROSS // 2,)),
            dma((banks // ACROSS // 2,)),
            dma((1,)),
            dma((1,)),
            dma((len(arrivals(chips)),)),
            dma((2,)),
            dma((2,)),
            pltpu.SemaphoreType.REGULAR((2,)),
        ],
        compiler_params=pltpu.CompilerParams(
            collective_id=0, has_side_effects=True, vmem_limit_bytes=24 * 1024 * 1024
        ),
    )(
        *(
            pltpu.with_memory_space_constraint(a, pltpu.HBM)
            for a in (
                master_down.reshape(total, width),
                router_weight.T,
                router_gain.reshape(1, LANES),
            )
        )
    )
    final, scale, router = pl.pallas_call(
        put_out,
        out_shape=tuple(jax.ShapeDtypeStruct(a.shape, a.dtype) for a in (final, scale, router)),
        in_specs=[pl.BlockSpec(memory_space=pltpu.VMEM)] * 3,
        out_specs=(pl.BlockSpec(memory_space=pltpu.HBM),) * 3,
        scratch_shapes=[dma((PUTS + 2,))],
        compiler_params=pltpu.CompilerParams(vmem_limit_bytes=1024 * 1024),
    )(final, scale, router)
    return final.reshape(experts, inner, width * zeros), scale, router.T


def solution(mesh):
    banks, zeros = mesh.shape["bank"], mesh.shape["zero"]
    return jax.shard_map(
        functools.partial(per_device, banks, zeros),
        mesh=mesh,
        in_specs=(P("bank", None, "zero"), P("zero", "bank"), P("zero")),
        out_specs=(P("bank", None, None), P("bank", None), P()),
        check_vma=False,
    )
```

```python
import functools

import jax
import jax.numpy as jnp
from jax import lax
from jax.experimental import pallas as pl
from jax.experimental.pallas import tpu as pltpu
from jax.sharding import PartitionSpec as P

MESH = pl.DeviceIdType.MESH
LANES = 128
ACROSS = 4
LOADS = 4
PUTS = 8
PIECES = (4, 4, 6, 2)
AHEAD = 2
QUARTER = PIECES[0]
EARLY = PIECES[AHEAD] * LANES
ORDER = ((0, 1, 2, 3), (0, 2, 3, 1))
ONWARD = ((0, 1), (2, 3))
TURNS = (1, 2, 3, 5, 7, 9, 11)


def arrivals(chips):
    keys = [
        (way, step, k)
        for way in (0, 1)
        for step in range(chips // 2)
        for k in range(len(PIECES))
        if step < chips // 2 - 1 or k in ONWARD[way]
    ]
    return {key: i for i, key in enumerate(keys)}


def kernel(
    banks, zeros, w_hbm, r_hbm, g_hbm, out, scale, router,
    w, r, g, early, lead, rest, shared, rows, parts, columns,
    load_sem, max_send, max_recv, part_send, part_recv, col_send, x_recv, y_recv,
    early_send, ring_send, ring_recv, pair_send, pair_recv, hello,
):
    total = w_hbm.shape[0]
    blocks = total // LANES
    chips, down = zeros // 2, banks // ACROSS
    far, number = chips // 2, arrivals(chips)
    bank, zero = lax.axis_index("bank"), lax.axis_index("zero")
    chip, core = zero // 2, lax.rem(zero, 2)
    partner = chip * 2 + 1 - core
    y, x = bank // ACROSS, lax.rem(bank, ACROSS)

    def shard_of(distance):
        return lax.rem(chip + distance + chips, chips) * 2 + core

    def along_x(distance):
        return y * ACROSS + lax.rem(x + distance + ACROSS, ACROSS)

    def along_y(distance):
        return lax.rem(y + distance + down, down)

    def remote(src, dst, send_sem, recv_sem, **device):
        return pltpu.make_async_remote_copy(
            src_ref=src, dst_ref=dst, send_sem=send_sem, recv_sem=recv_sem,
            device_id=device, device_id_type=MESH,
        )

    offsets = sorted(range(1, chips), key=lambda o: -min(o, chips - o))
    peers = [lax.rem(chip + o, chips) * 2 + c for o in offsets for c in (core, 1 - core)]
    peers.append(partner)
    barrier = pltpu.get_barrier_semaphore()
    for peer in peers:
        pl.semaphore_signal(barrier, inc=1, device_id={"zero": peer}, device_id_type=MESH)

    share = total // LOADS

    def load(i):
        at = pl.ds(i * share, share)
        return pltpu.make_async_copy(w_hbm.at[at], w.at[at], load_sem.at[i])

    load_r = pltpu.make_async_copy(r_hbm, r, load_sem.at[LOADS])
    load_g = pltpu.make_async_copy(g_hbm, g, load_sem.at[LOADS + 1])
    for i in range(LOADS):
        load(i).start()
    load_r.start()
    load_g.start()

    sides = (
        (x, ACROSS, lambda to: to + y * ACROSS, hello.at[0]),
        (y, down, lambda to: to * ACROSS + x, hello.at[1]),
    )

    def to_higher(here, size, bank_of, signal):
        @pl.when(here < size - 1)
        def _():
            signal(bank_of(here + 1))

        if size > 2:

            @pl.when(here == 0)
            def _():
                signal(bank_of(size - 1))

    def to_lower(here, size, bank_of, signal):
        @pl.when(here > 0)
        def _():
            signal(bank_of(here - 1))

        if size > 2:

            @pl.when(here == size - 1)
            def _():
                signal(bank_of(0))

    def lower(here, size):
        return (here + size - 1) // size + ((here + 1) // size if size > 2 else 0)

    def higher(here, size):
        return (2 if size > 2 else 1) - lower(here, size)

    def answers(here, size, sem):
        @pl.when(higher(here, size) > 0)
        def _():
            pl.semaphore_wait(sem, higher(here, size))

    for here, size, bank_of, _ in sides:
        to_higher(
            here, size, bank_of,
            lambda to: pl.semaphore_signal(
                barrier, inc=1, device_id={"bank": to}, device_id_type=MESH
            ),
        )

    for i in range(LOADS):
        load(i).wait()
        for j in range(i * blocks // LOADS, (i + 1) * blocks // LOADS):
            block = jnp.abs(w[j * LANES : (j + 1) * LANES, :])
            q, k = j // QUARTER, j % QUARTER
            row = jnp.max(block.T, axis=0, keepdims=True)
            if q == 0:
                lead[zero, k : k + 1, :] = row
            else:
                rest[zero, q - 1, k : k + 1, :] = row
    load_r.wait()
    load_g.wait()
    product = r[...] * g[...]
    parts[zero, :, 0:LANES] = product[0:1]
    parts[zero, :, LANES : 2 * LANES] = product[1:2]

    pl.semaphore_wait(barrier, zeros - 1 + lower(x, ACROSS) + lower(y, down))

    mine = lead.at[zero]
    for peer in peers:
        remote(mine, mine, max_send.at[0], max_recv.at[0], zero=peer).start()
    mine = rest.at[zero]
    for peer in peers[0:-1:2]:
        remote(mine, mine, max_send.at[1], max_recv.at[1], zero=peer).start()

    right, left = shard_of(1), shard_of(-1)
    starts = [sum(PIECES[:k]) for k in range(len(PIECES) + 1)]

    def first_rows(way):
        return remote(
            w.at[pl.ds(starts[AHEAD] * LANES, EARLY)], early.at[way], early_send.at[0],
            ring_recv.at[number[way, 0, AHEAD]], zero=(right, left)[way],
        )

    @pl.when(core == 0)
    def _():
        first_rows(0).start()
        first_rows(1).start()

    for peer in peers:
        mine = parts.at[zero]
        remote(mine, mine, part_send.at[0], part_recv.at[0], zero=peer).start()
    for here, size, bank_of, sem in sides:
        to_lower(
            here, size, bank_of,
            lambda to: pl.semaphore_signal(
                sem, inc=1, device_id={"bank": to}, device_id_type=MESH
            ),
        )

    def piece(shard, k):
        return out.at[
            pl.ds(starts[k] * LANES, PIECES[k] * LANES),
            pl.ds(pl.multiple_of(shard * LANES, LANES), LANES),
        ]

    def hop(way, step, shard, k):
        at = piece(shard, k)
        sem = early_send if step == 0 and k == AHEAD else ring_send
        return remote(
            at, at, sem.at[0], ring_recv.at[number[way, step, k]], zero=(right, left)[way]
        )

    def pair(shard, k):
        at = piece(shard, k)
        return remote(at, at, pair_send.at[0], pair_recv.at[0], zero=partner)

    def divide(k, shard=zero, source=w, first=0):
        for j in range(starts[k], starts[k + 1]):
            at, source_at = pl.ds(j * LANES, LANES), pl.ds((j - first) * LANES, LANES)
            by = jnp.broadcast_to(rows[j : j + 1, :], (LANES, LANES)).T
            to = pl.ds(pl.multiple_of(shard * LANES, LANES), LANES)
            out[at, to] = (source[source_at, :] / by).astype(jnp.bfloat16)

    others = lead.at[pl.ds(0, zeros - 1)]
    remote(others, others, max_send.at[0], max_recv.at[0], zero=partner).wait_recv()
    most = lead[0]
    for i in range(1, zeros):
        most = jnp.maximum(most, lead[i])
    rows[0:QUARTER, :] = most
    divide(0)
    hop(0, 0, zero, 0).start()
    hop(1, 0, zero, 0).start()

    others = rest.at[pl.ds(0, chips - 1)]
    remote(others, others, max_send.at[1], max_recv.at[1], zero=partner).wait_recv()
    most = rest[core]
    for i in range(1, chips):
        most = jnp.maximum(most, rest[2 * i + core])
    shared[core] = most
    ours = shared.at[core]
    share_max = remote(ours, ours, pair_send.at[1], pair_recv.at[1], zero=partner)
    share_max.start()
    share_max.wait_recv()
    for q in range(1, blocks // QUARTER):
        rows[q * QUARTER : (q + 1) * QUARTER, :] = jnp.maximum(
            shared[0, q - 1], shared[1, q - 1]
        )
    divide(1)
    hop(0, 0, zero, 1).start()
    divide(AHEAD)

    @pl.when(core == 1)
    def _():
        hop(1, 0, zero, AHEAD).start()
        hop(0, 0, zero, AHEAD).start()

    divide(3)
    hop(1, 0, zero, 3).start()
    hop(0, 0, zero, 3).start()
    hop(1, 0, zero, 1).start()
    for k in range(len(PIECES)):
        pair(zero, k).start()

    per_expert = blocks // scale.shape[0]
    for j in range(blocks):
        e, at = j // per_expert, (j % per_expert) * LANES
        scale[e : e + 1, at : at + LANES] = rows[j : j + 1, :]

    def banks_of(first, count):
        size = count * 2 * zeros
        return columns.at[pl.ds(pl.multiple_of(first * 2 * zeros, 2 * zeros), size)]

    def send_x(distance, peer):
        at = banks_of(along_x(distance), 1)
        return remote(at, at, col_send.at[0], x_recv.at[abs(distance) - 1], bank=peer)

    def x_first():
        others = parts.at[pl.ds(0, zeros - 1)]
        remote(others, others, part_send.at[0], part_recv.at[0], zero=partner).wait_recv()
        tile = pl.multiple_of(bank * 2 * zeros, 2 * zeros)
        for i in range(zeros):
            columns[pl.ds(tile + i, 1), :] = parts[i, :, 0:LANES]
            columns[pl.ds(tile + zeros + i, 1), :] = parts[i, :, LANES : 2 * LANES]
        answers(x, ACROSS, hello.at[0])
        at = banks_of(bank, 1)
        remote(at, at, col_send.at[0], x_recv.at[0], bank=along_x(1)).start()
        remote(at, at, col_send.at[0], x_recv.at[0], bank=along_x(-1)).start()

    def x_second():
        both = banks_of(0, 2)
        remote(both, both, col_send.at[0], x_recv.at[0], bank=along_x(1)).wait_recv()
        at = banks_of(along_x(-1), 1)
        remote(at, at, col_send.at[0], x_recv.at[1], bank=along_x(1)).start()

    ups, downs = down // 2, (down - 1) // 2

    def y_step(step):
        if step == 0:
            send_x(2, along_x(1)).wait_recv()
            answers(y, down, hello.at[1])
        if 1 <= step <= ups:
            came = banks_of(0, (2 if step <= downs else 1) * ACROSS)
            remote(
                came, came, col_send.at[0], y_recv.at[step - 1], bank=along_x(1)
            ).wait_recv()
        if step < ups:
            at = banks_of(along_y(-step) * ACROSS, ACROSS)
            remote(
                at, at, col_send.at[0], y_recv.at[step],
                bank=along_y(1) * ACROSS + x,
            ).start()
        if step < downs:
            at = banks_of(along_y(step) * ACROSS, ACROSS)
            remote(
                at, at, col_send.at[0], y_recv.at[step],
                bank=along_y(-1) * ACROSS + x,
            ).start()

    def finish_router():
        for i in range(zeros):
            router[:, i * LANES : (i + 1) * LANES] = columns[
                pl.ds(i, 2 * banks, stride=zeros), :
            ].astype(jnp.bfloat16)

    stages = [x_first, x_second] + [functools.partial(y_step, step) for step in range(ups + 1)]

    def forward(way, step, k, onward):
        shard = shard_of(-step if way == 0 else step)
        hop(way, step - 1, shard, k).wait_recv()
        if onward:
            hop(way, step, shard, k).start()
        pair(shard, k).start()

    def forward_early(way):
        shard = shard_of(-1 if way == 0 else 1)
        first_rows(way).wait_recv()
        divide(AHEAD, shard, early.at[way], starts[AHEAD])
        hop(way, 1, shard, AHEAD).start()
        pair(shard, AHEAD).start()

    @pl.when(core == 0)
    def _():
        forward_early(0)
        forward_early(1)

    turn = 0
    for step in range(1, far):
        for i in range(len(PIECES)):
            for way in (0, 1):
                k = ORDER[way][i]
                if step == 1 and k == AHEAD:
                    pl.when(core == 1)(functools.partial(forward, way, step, k, True))
                else:
                    forward(way, step, k, step < far - 1 or k in ONWARD[way])
            if turn in TURNS and stages:
                stages.pop(0)()
            turn += 1
    for stage in stages:
        stage()
    finish_router()
    for i in range(len(ONWARD[0])):
        for way in (0, 1):
            forward(way, far, ONWARD[way][i], False)

    size = ((chips - 1) * total - 2 * EARLY) // chips
    sent = out.at[pl.ds(0, size), pl.ds(0, chips * LANES)]
    remote(sent, sent, ring_send.at[0], pair_recv.at[0], zero=right).wait_send()

    @pl.when(core == 0)
    def _():
        remote(early, early, early_send.at[0], pair_recv.at[0], zero=right).wait_send()

    @pl.when(core == 1)
    def _():
        sent = out.at[pl.ds(0, 2 * EARLY), pl.ds(0, LANES)]
        remote(sent, sent, early_send.at[0], pair_recv.at[0], zero=right).wait_send()

    others = lead.at[pl.ds(0, zeros - 1)]
    remote(others, others, max_send.at[0], max_recv.at[0], zero=partner).wait_send()
    others = rest.at[pl.ds(0, chips - 1)]
    remote(others, others, max_send.at[1], max_recv.at[1], zero=partner).wait_send()
    share_max.wait_send()
    others = parts.at[pl.ds(0, zeros - 1)]
    remote(others, others, part_send.at[0], part_recv.at[0], zero=partner).wait_send()
    size = (ACROSS - 1 + (down - 1) * ACROSS) * 2 * zeros
    others = columns.at[pl.ds(0, size)]
    remote(others, others, col_send.at[0], x_recv.at[0], bank=along_x(1)).wait_send()
    both = out.at[:, pl.ds(0, chips * LANES)]
    remote(both, both, pair_send.at[0], pair_recv.at[0], zero=partner).wait()


def put_out(final, scale, router, final_hbm, scale_hbm, router_hbm, sem):
    share = final.shape[0] // PUTS
    copies = [
        pltpu.make_async_copy(
            final.at[pl.ds(i * share, share)], final_hbm.at[pl.ds(i * share, share)], sem.at[i]
        )
        for i in range(PUTS)
    ]
    copies.append(pltpu.make_async_copy(scale, scale_hbm, sem.at[PUTS]))
    copies.append(pltpu.make_async_copy(router, router_hbm, sem.at[PUTS + 1]))
    for copy in copies:
        copy.start()
    for copy in copies:
        copy.wait()


def per_device(banks, zeros, master_down, router_weight, router_gain):
    experts, inner, width = master_down.shape
    total = experts * inner
    chips, quarters = zeros // 2, total // LANES // QUARTER
    dma = pltpu.SemaphoreType.DMA
    final, scale, router = pl.pallas_call(
        functools.partial(kernel, banks, zeros),
        out_shape=(
            jax.ShapeDtypeStruct((total, width * zeros), jnp.bfloat16),
            jax.ShapeDtypeStruct((experts, inner), jnp.float32),
            jax.ShapeDtypeStruct((2 * banks, LANES * zeros), jnp.bfloat16),
        ),
        in_specs=[pl.BlockSpec(memory_space=pltpu.HBM)] * 3,
        out_specs=(pl.BlockSpec(memory_space=pltpu.VMEM),) * 3,
        scratch_shapes=[
            pltpu.VMEM((total, LANES), jnp.float32),
            pltpu.VMEM((2, LANES), jnp.float32),
            pltpu.VMEM((1, LANES), jnp.float32),
            pltpu.VMEM((2, EARLY, LANES), jnp.float32),
            pltpu.VMEM((zeros, QUARTER, LANES), jnp.float32),
            pltpu.VMEM((zeros, quarters - 1, QUARTER, LANES), jnp.float32),
            pltpu.VMEM((2, quarters - 1, QUARTER, LANES), jnp.float32),
            pltpu.VMEM((total // LANES, LANES), jnp.float32),
            pltpu.VMEM((zeros, 1, 2 * LANES), jnp.float32),
            pltpu.VMEM((2 * banks * zeros, LANES), jnp.float32),
            dma((LOADS + 2,)),
            dma((2,)),
            dma((2,)),
            dma((1,)),
            dma((1,)),
            dma((1,)),
            dma((ACROSS // 2,)),
            dma((banks // ACROSS // 2,)),
            dma((1,)),
            dma((1,)),
            dma((len(arrivals(chips)),)),
            dma((2,)),
            dma((2,)),
            pltpu.SemaphoreType.REGULAR((2,)),
        ],
        compiler_params=pltpu.CompilerParams(
            collective_id=0, has_side_effects=True, vmem_limit_bytes=24 * 1024 * 1024
        ),
    )(
        *(
            pltpu.with_memory_space_constraint(a, pltpu.HBM)
            for a in (
                master_down.reshape(total, width),
                router_weight.T,
                router_gain.reshape(1, LANES),
            )
        )
    )
    final, scale, router = pl.pallas_call(
        put_out,
        out_shape=tuple(jax.ShapeDtypeStruct(a.shape, a.dtype) for a in (final, scale, router)),
        in_specs=[pl.BlockSpec(memory_space=pltpu.VMEM)] * 3,
        out_specs=(pl.BlockSpec(memory_space=pltpu.HBM),) * 3,
        scratch_shapes=[dma((PUTS + 2,))],
        compiler_params=pltpu.CompilerParams(vmem_limit_bytes=1024 * 1024),
    )(final, scale, router)
    return final.reshape(experts, inner, width * zeros), scale, router.T


def solution(mesh):
    banks, zeros = mesh.shape["bank"], mesh.shape["zero"]
    return jax.shard_map(
        functools.partial(per_device, banks, zeros),
        mesh=mesh,
        in_specs=(P("bank", None, "zero"), P("zero", "bank"), P("zero")),
        out_specs=(P("bank", None, None), P("bank", None), P()),
        check_vma=False,
    )
```

```python
import functools

import jax
import jax.numpy as jnp
from jax import lax
from jax.experimental import pallas as pl
from jax.experimental.pallas import tpu as pltpu
from jax.sharding import PartitionSpec as P

MESH = pl.DeviceIdType.MESH
LANES = 128
ACROSS = 4
LOADS = 4
PUTS = 8
PIECES = (4, 4, 6, 2)
AHEAD = 2
QUARTER = PIECES[0]
EARLY = PIECES[AHEAD] * LANES
ORDER = ((0, 1, 2, 3), (0, 2, 3, 1))
ONWARD = ((0, 1), (2, 3))
TURNS = (1, 3, 4, 6, 8, 9, 11)


def arrivals(chips):
    keys = [
        (way, step, k)
        for way in (0, 1)
        for step in range(chips // 2)
        for k in range(len(PIECES))
        if step < chips // 2 - 1 or k in ONWARD[way]
    ]
    return {key: i for i, key in enumerate(keys)}


def kernel(
    banks, zeros, w_hbm, r_hbm, g_hbm, out, scale, router,
    w, r, g, early, lead, rest, shared, rows, parts, columns,
    load_sem, max_send, max_recv, part_send, part_recv, col_send, x_recv, y_recv,
    early_send, ring_send, ring_recv, pair_send, pair_recv, hello,
):
    total = w_hbm.shape[0]
    blocks = total // LANES
    chips, down = zeros // 2, banks // ACROSS
    far, number = chips // 2, arrivals(chips)
    bank, zero = lax.axis_index("bank"), lax.axis_index("zero")
    chip, core = zero // 2, lax.rem(zero, 2)
    partner = chip * 2 + 1 - core
    y, x = bank // ACROSS, lax.rem(bank, ACROSS)

    def shard_of(distance):
        return lax.rem(chip + distance + chips, chips) * 2 + core

    def along_x(distance):
        return y * ACROSS + lax.rem(x + distance + ACROSS, ACROSS)

    def along_y(distance):
        return lax.rem(y + distance + down, down)

    def remote(src, dst, send_sem, recv_sem, **device):
        return pltpu.make_async_remote_copy(
            src_ref=src, dst_ref=dst, send_sem=send_sem, recv_sem=recv_sem,
            device_id=device, device_id_type=MESH,
        )

    offsets = sorted(range(1, chips), key=lambda o: -min(o, chips - o))
    peers = [lax.rem(chip + o, chips) * 2 + c for o in offsets for c in (core, 1 - core)]
    peers.append(partner)
    barrier = pltpu.get_barrier_semaphore()
    for peer in peers:
        pl.semaphore_signal(barrier, inc=1, device_id={"zero": peer}, device_id_type=MESH)

    share = total // LOADS

    def load(i):
        at = pl.ds(i * share, share)
        return pltpu.make_async_copy(w_hbm.at[at], w.at[at], load_sem.at[i])

    load_r = pltpu.make_async_copy(r_hbm, r, load_sem.at[LOADS])
    load_g = pltpu.make_async_copy(g_hbm, g, load_sem.at[LOADS + 1])
    for i in range(LOADS):
        load(i).start()
    load_r.start()
    load_g.start()

    sides = (
        (x, ACROSS, lambda to: to + y * ACROSS, hello.at[0]),
        (y, down, lambda to: to * ACROSS + x, hello.at[1]),
    )

    def to_higher(here, size, bank_of, signal):
        @pl.when(here < size - 1)
        def _():
            signal(bank_of(here + 1))

        if size > 2:

            @pl.when(here == 0)
            def _():
                signal(bank_of(size - 1))

    def to_lower(here, size, bank_of, signal):
        @pl.when(here > 0)
        def _():
            signal(bank_of(here - 1))

        if size > 2:

            @pl.when(here == size - 1)
            def _():
                signal(bank_of(0))

    def lower(here, size):
        return (here + size - 1) // size + ((here + 1) // size if size > 2 else 0)

    def higher(here, size):
        return (2 if size > 2 else 1) - lower(here, size)

    def answers(here, size, sem):
        @pl.when(higher(here, size) > 0)
        def _():
            pl.semaphore_wait(sem, higher(here, size))

    for here, size, bank_of, _ in sides:
        to_higher(
            here, size, bank_of,
            lambda to: pl.semaphore_signal(
                barrier, inc=1, device_id={"bank": to}, device_id_type=MESH
            ),
        )

    for i in range(LOADS):
        load(i).wait()
        for j in range(i * blocks // LOADS, (i + 1) * blocks // LOADS):
            block = jnp.abs(w[j * LANES : (j + 1) * LANES, :])
            q, k = j // QUARTER, j % QUARTER
            row = jnp.max(block.T, axis=0, keepdims=True)
            if q == 0:
                lead[zero, k : k + 1, :] = row
            else:
                rest[zero, q - 1, k : k + 1, :] = row
    load_r.wait()
    load_g.wait()
    product = r[...] * g[...]
    parts[zero, :, 0:LANES] = product[0:1]
    parts[zero, :, LANES : 2 * LANES] = product[1:2]

    pl.semaphore_wait(barrier, zeros - 1 + lower(x, ACROSS) + lower(y, down))

    mine = lead.at[zero]
    for peer in peers:
        remote(mine, mine, max_send.at[0], max_recv.at[0], zero=peer).start()
    mine = rest.at[zero]
    for peer in peers[0:-1:2]:
        remote(mine, mine, max_send.at[1], max_recv.at[1], zero=peer).start()

    right, left = shard_of(1), shard_of(-1)
    starts = [sum(PIECES[:k]) for k in range(len(PIECES) + 1)]

    def first_rows(way):
        return remote(
            w.at[pl.ds(starts[AHEAD] * LANES, EARLY)], early.at[way], early_send.at[0],
            ring_recv.at[number[way, 0, AHEAD]], zero=(right, left)[way],
        )

    @pl.when(core == 0)
    def _():
        first_rows(0).start()
        first_rows(1).start()

    for peer in peers:
        mine = parts.at[zero]
        remote(mine, mine, part_send.at[0], part_recv.at[0], zero=peer).start()
    for here, size, bank_of, sem in sides:
        to_lower(
            here, size, bank_of,
            lambda to: pl.semaphore_signal(
                sem, inc=1, device_id={"bank": to}, device_id_type=MESH
            ),
        )

    def piece(shard, k):
        return out.at[
            pl.ds(starts[k] * LANES, PIECES[k] * LANES),
            pl.ds(pl.multiple_of(shard * LANES, LANES), LANES),
        ]

    def hop(way, step, shard, k):
        at = piece(shard, k)
        sem = early_send if step == 0 and k == AHEAD else ring_send
        return remote(
            at, at, sem.at[0], ring_recv.at[number[way, step, k]], zero=(right, left)[way]
        )

    def pair(shard, k):
        at = piece(shard, k)
        return remote(at, at, pair_send.at[0], pair_recv.at[0], zero=partner)

    def divide(k, shard=zero, source=w, first=0):
        for j in range(starts[k], starts[k + 1]):
            at, source_at = pl.ds(j * LANES, LANES), pl.ds((j - first) * LANES, LANES)
            by = jnp.broadcast_to(rows[j : j + 1, :], (LANES, LANES)).T
            to = pl.ds(pl.multiple_of(shard * LANES, LANES), LANES)
            out[at, to] = (source[source_at, :] / by).astype(jnp.bfloat16)

    others = lead.at[pl.ds(0, zeros - 1)]
    remote(others, others, max_send.at[0], max_recv.at[0], zero=partner).wait_recv()
    most = lead[0]
    for i in range(1, zeros):
        most = jnp.maximum(most, lead[i])
    rows[0:QUARTER, :] = most
    divide(0)
    hop(0, 0, zero, 0).start()
    hop(1, 0, zero, 0).start()

    others = rest.at[pl.ds(0, chips - 1)]
    remote(others, others, max_send.at[1], max_recv.at[1], zero=partner).wait_recv()
    most = rest[core]
    for i in range(1, chips):
        most = jnp.maximum(most, rest[2 * i + core])
    shared[core] = most
    ours = shared.at[core]
    share_max = remote(ours, ours, pair_send.at[1], pair_recv.at[1], zero=partner)
    share_max.start()
    share_max.wait_recv()
    for q in range(1, blocks // QUARTER):
        rows[q * QUARTER : (q + 1) * QUARTER, :] = jnp.maximum(
            shared[0, q - 1], shared[1, q - 1]
        )
    divide(1)
    hop(0, 0, zero, 1).start()
    divide(AHEAD)

    @pl.when(core == 1)
    def _():
        hop(1, 0, zero, AHEAD).start()
        hop(0, 0, zero, AHEAD).start()

    divide(3)
    hop(1, 0, zero, 3).start()
    hop(0, 0, zero, 3).start()
    hop(1, 0, zero, 1).start()
    for k in range(len(PIECES)):
        pair(zero, k).start()

    per_expert = blocks // scale.shape[0]
    for j in range(blocks):
        e, at = j // per_expert, (j % per_expert) * LANES
        scale[e : e + 1, at : at + LANES] = rows[j : j + 1, :]

    def banks_of(first, count):
        size = count * 2 * zeros
        return columns.at[pl.ds(pl.multiple_of(first * 2 * zeros, 2 * zeros), size)]

    def send_x(distance, peer):
        at = banks_of(along_x(distance), 1)
        return remote(at, at, col_send.at[0], x_recv.at[abs(distance) - 1], bank=peer)

    def x_first():
        others = parts.at[pl.ds(0, zeros - 1)]
        remote(others, others, part_send.at[0], part_recv.at[0], zero=partner).wait_recv()
        tile = pl.multiple_of(bank * 2 * zeros, 2 * zeros)
        for i in range(zeros):
            columns[pl.ds(tile + i, 1), :] = parts[i, :, 0:LANES]
            columns[pl.ds(tile + zeros + i, 1), :] = parts[i, :, LANES : 2 * LANES]
        answers(x, ACROSS, hello.at[0])
        at = banks_of(bank, 1)
        remote(at, at, col_send.at[0], x_recv.at[0], bank=along_x(1)).start()
        remote(at, at, col_send.at[0], x_recv.at[0], bank=along_x(-1)).start()

    def x_second():
        both = banks_of(0, 2)
        remote(both, both, col_send.at[0], x_recv.at[0], bank=along_x(1)).wait_recv()
        at = banks_of(along_x(-1), 1)
        remote(at, at, col_send.at[0], x_recv.at[1], bank=along_x(1)).start()

    ups, downs = down // 2, (down - 1) // 2

    def y_step(step):
        if step == 0:
            send_x(2, along_x(1)).wait_recv()
            answers(y, down, hello.at[1])
        if 1 <= step <= ups:
            came = banks_of(0, (2 if step <= downs else 1) * ACROSS)
            remote(
                came, came, col_send.at[0], y_recv.at[step - 1], bank=along_x(1)
            ).wait_recv()
        if step < ups:
            at = banks_of(along_y(-step) * ACROSS, ACROSS)
            remote(
                at, at, col_send.at[0], y_recv.at[step],
                bank=along_y(1) * ACROSS + x,
            ).start()
        if step < downs:
            at = banks_of(along_y(step) * ACROSS, ACROSS)
            remote(
                at, at, col_send.at[0], y_recv.at[step],
                bank=along_y(-1) * ACROSS + x,
            ).start()

    def finish_router():
        for i in range(zeros):
            router[:, i * LANES : (i + 1) * LANES] = columns[
                pl.ds(i, 2 * banks, stride=zeros), :
            ].astype(jnp.bfloat16)

    stages = [x_first, x_second] + [functools.partial(y_step, step) for step in range(ups + 1)]

    def forward(way, step, k, onward):
        shard = shard_of(-step if way == 0 else step)
        hop(way, step - 1, shard, k).wait_recv()
        if onward:
            hop(way, step, shard, k).start()
        pair(shard, k).start()

    def forward_early(way):
        shard = shard_of(-1 if way == 0 else 1)
        first_rows(way).wait_recv()
        divide(AHEAD, shard, early.at[way], starts[AHEAD])
        hop(way, 1, shard, AHEAD).start()
        pair(shard, AHEAD).start()

    @pl.when(core == 0)
    def _():
        forward_early(0)
        forward_early(1)

    turn = 0
    for step in range(1, far):
        for i in range(len(PIECES)):
            for way in (0, 1):
                k = ORDER[way][i]
                if step == 1 and k == AHEAD:
                    pl.when(core == 1)(functools.partial(forward, way, step, k, True))
                else:
                    forward(way, step, k, step < far - 1 or k in ONWARD[way])
            if turn in TURNS and stages:
                stages.pop(0)()
            turn += 1
    for stage in stages:
        stage()
    finish_router()
    for i in range(len(ONWARD[0])):
        for way in (0, 1):
            forward(way, far, ONWARD[way][i], False)

    size = ((chips - 1) * total - 2 * EARLY) // chips
    sent = out.at[pl.ds(0, size), pl.ds(0, chips * LANES)]
    remote(sent, sent, ring_send.at[0], pair_recv.at[0], zero=right).wait_send()

    @pl.when(core == 0)
    def _():
        remote(early, early, early_send.at[0], pair_recv.at[0], zero=right).wait_send()

    @pl.when(core == 1)
    def _():
        sent = out.at[pl.ds(0, 2 * EARLY), pl.ds(0, LANES)]
        remote(sent, sent, early_send.at[0], pair_recv.at[0], zero=right).wait_send()

    others = lead.at[pl.ds(0, zeros - 1)]
    remote(others, others, max_send.at[0], max_recv.at[0], zero=partner).wait_send()
    others = rest.at[pl.ds(0, chips - 1)]
    remote(others, others, max_send.at[1], max_recv.at[1], zero=partner).wait_send()
    share_max.wait_send()
    others = parts.at[pl.ds(0, zeros - 1)]
    remote(others, others, part_send.at[0], part_recv.at[0], zero=partner).wait_send()
    size = (ACROSS - 1 + (down - 1) * ACROSS) * 2 * zeros
    others = columns.at[pl.ds(0, size)]
    remote(others, others, col_send.at[0], x_recv.at[0], bank=along_x(1)).wait_send()
    both = out.at[:, pl.ds(0, chips * LANES)]
    remote(both, both, pair_send.at[0], pair_recv.at[0], zero=partner).wait()


def put_out(final, scale, router, final_hbm, scale_hbm, router_hbm, sem):
    share = final.shape[0] // PUTS
    copies = [
        pltpu.make_async_copy(
            final.at[pl.ds(i * share, share)], final_hbm.at[pl.ds(i * share, share)], sem.at[i]
        )
        for i in range(PUTS)
    ]
    copies.append(pltpu.make_async_copy(scale, scale_hbm, sem.at[PUTS]))
    copies.append(pltpu.make_async_copy(router, router_hbm, sem.at[PUTS + 1]))
    for copy in copies:
        copy.start()
    for copy in copies:
        copy.wait()


def per_device(banks, zeros, master_down, router_weight, router_gain):
    experts, inner, width = master_down.shape
    total = experts * inner
    chips, quarters = zeros // 2, total // LANES // QUARTER
    dma = pltpu.SemaphoreType.DMA
    final, scale, router = pl.pallas_call(
        functools.partial(kernel, banks, zeros),
        out_shape=(
            jax.ShapeDtypeStruct((total, width * zeros), jnp.bfloat16),
            jax.ShapeDtypeStruct((experts, inner), jnp.float32),
            jax.ShapeDtypeStruct((2 * banks, LANES * zeros), jnp.bfloat16),
        ),
        in_specs=[pl.BlockSpec(memory_space=pltpu.HBM)] * 3,
        out_specs=(pl.BlockSpec(memory_space=pltpu.VMEM),) * 3,
        scratch_shapes=[
            pltpu.VMEM((total, LANES), jnp.float32),
            pltpu.VMEM((2, LANES), jnp.float32),
            pltpu.VMEM((1, LANES), jnp.float32),
            pltpu.VMEM((2, EARLY, LANES), jnp.float32),
            pltpu.VMEM((zeros, QUARTER, LANES), jnp.float32),
            pltpu.VMEM((zeros, quarters - 1, QUARTER, LANES), jnp.float32),
            pltpu.VMEM((2, quarters - 1, QUARTER, LANES), jnp.float32),
            pltpu.VMEM((total // LANES, LANES), jnp.float32),
            pltpu.VMEM((zeros, 1, 2 * LANES), jnp.float32),
            pltpu.VMEM((2 * banks * zeros, LANES), jnp.float32),
            dma((LOADS + 2,)),
            dma((2,)),
            dma((2,)),
            dma((1,)),
            dma((1,)),
            dma((1,)),
            dma((ACROSS // 2,)),
            dma((banks // ACROSS // 2,)),
            dma((1,)),
            dma((1,)),
            dma((len(arrivals(chips)),)),
            dma((2,)),
            dma((2,)),
            pltpu.SemaphoreType.REGULAR((2,)),
        ],
        compiler_params=pltpu.CompilerParams(
            collective_id=0, has_side_effects=True, vmem_limit_bytes=24 * 1024 * 1024
        ),
    )(
        *(
            pltpu.with_memory_space_constraint(a, pltpu.HBM)
            for a in (
                master_down.reshape(total, width),
                router_weight.T,
                router_gain.reshape(1, LANES),
            )
        )
    )
    final, scale, router = pl.pallas_call(
        put_out,
        out_shape=tuple(jax.ShapeDtypeStruct(a.shape, a.dtype) for a in (final, scale, router)),
        in_specs=[pl.BlockSpec(memory_space=pltpu.VMEM)] * 3,
        out_specs=(pl.BlockSpec(memory_space=pltpu.HBM),) * 3,
        scratch_shapes=[dma((PUTS + 2,))],
        compiler_params=pltpu.CompilerParams(vmem_limit_bytes=1024 * 1024),
    )(final, scale, router)
    return final.reshape(experts, inner, width * zeros), scale, router.T


def solution(mesh):
    banks, zeros = mesh.shape["bank"], mesh.shape["zero"]
    return jax.shard_map(
        functools.partial(per_device, banks, zeros),
        mesh=mesh,
        in_specs=(P("bank", None, "zero"), P("zero", "bank"), P("zero")),
        out_specs=(P("bank", None, None), P("bank", None), P()),
        check_vma=False,
    )
```
